32 devices in a mesh: ctx: 16 (over z, x, core), fsdp: 2 (over y).
Axes of the slice: x: 2, y: 2, z: 4, core: 2. Of those that a mesh axis runs over, the one named last changes fastest.
Arguments:
- layer_input: bfloat16 [2048, 4096], P('ctx'), may hold values from -8 to 8
- gain: float32 [4096], replicated, may hold values from 0.5 to 1.5
- codes: int32 [4096, 384], P('fsdp'), may hold values from -2147483648 to 2147483646
- column_scale_quantized: int32 [64, 3072], P('fsdp'), may hold values from 0 to 255
- block_second_scale: float32 [64], replicated, may hold values from 0.03 to 0.12
- query_down_map: bfloat16 [4096, 16], replicated, may hold values from -0.09375 to 0.09375
- query_up_map: bfloat16 [16, 2048], P(None, 'fsdp'), may hold values from -0.29882812 to 0.29882812
- token_document: int32 [2048], P('ctx'), may hold values from 0 to 3, as said below
- output_cotangent: bfloat16 [2048, 2048], P('ctx', 'fsdp'), may hold values from -0.059814453 to 0.059814453
Outputs:
- attn: bfloat16 [2048, 2048], P('ctx', 'fsdp')
- grad_a: float32 [4096, 16], replicated
- up_map_gradient: float32 [16, 2048], P(None, 'fsdp')
The draws below stay inside these ranges and needn't reach their ends.
Inputs may be any that keep to these rules, and one draw needn't show every extreme that they name: token_document never falls along the sequence; each document has 1 to 1536 tokens and one has exactly 1536.
All inputs are finite; a program needn't handle non-finite values.
Results may differ from the reference program's by a relative error of at most 0.028.
Values may be sent and summed in bfloat16 or wider, within the bound.
A program may use at most 192 MiB of HBM per device.

```python
import math
import jax
import jax.numpy as jnp
import numpy as np
from jax import lax

MODEL_WIDTH = 4096
QUERY_HEADS = 16
KEY_VALUE_HEADS = 4
HEAD_SIZE = 128
ADAPTER_RANK = 16
DOCS = 4
SEQUENCE_TOKENS = 2048
MOST = 1536
QUERY_FEATURES = 2048
COLS = 3072
N_FSDP = 2


NF4_LEVELS = [-1.0, -0.6961928009986877, -0.5250730514526367, -0.39491748809814453, -0.28444138169288635, -0.18477343022823334, -0.09105003625154495, 0.0, 0.07958029955625534, 0.16093020141124725, 0.24611230194568634, 0.33791524171829224, 0.44070982933044434, 0.5626170039176941, 0.7229568362236023, 1.0]


def weight_parts(key):
    code_key = jax.random.fold_in(key, 101)
    scale_key = jax.random.fold_in(key, 102)
    const_key = jax.random.fold_in(key, 103)
    packed = jax.random.randint(code_key, (MODEL_WIDTH, COLS // 8), -2147483648, 2147483647, dtype=jnp.int32)
    scales = jax.random.randint(scale_key, (MODEL_WIDTH // 64, COLS), 0, 256, dtype=jnp.int32)
    lower, upper = (0.03, 0.09)
    consts = jnp.exp(jax.random.uniform(const_key, (MODEL_WIDTH // 64,), jnp.float32, math.log(lower), math.log(upper)))
    return (packed, scales, consts)


def unpack_weights(packed, scales, consts):
    row_count = packed.shape[0]
    pieces = [jnp.bitwise_and(jnp.right_shift(packed, 4 * nibble), 15) for nibble in range(8)]
    unpacked = jnp.stack(pieces, axis=-1).reshape(row_count, packed.shape[1] * 8)
    table = jnp.asarray(NF4_LEVELS, jnp.float32)
    levels = table[unpacked]
    absmax = (scales.astype(jnp.float32) + 1.0) / 256.0 * consts[:, None]
    return (levels.reshape(row_count // 64, 64, -1) * absmax[:, None, :]).reshape(row_count, -1)


def doc_layout(key):
    layout_key = jax.random.fold_in(key, 401)
    long_slot = jax.random.randint(jax.random.fold_in(layout_key, 1), (), 1, DOCS, dtype=jnp.int32)
    remaining = jnp.int32(SEQUENCE_TOKENS - MOST)
    others = []
    for number in range(DOCS - 2):
        upper_len = remaining - (DOCS - 2 - number) + 1
        length_now = jax.random.randint(jax.random.fold_in(layout_key, 10 + number), (), 1, upper_len, dtype=jnp.int32)
        others.append(length_now)
        remaining = remaining - length_now
    others.append(remaining)
    lengths = []
    for number in range(DOCS):
        before = others[min(number, DOCS - 2)]
        after = others[max(number - 1, 0)]
        lengths.append(jnp.where(number < long_slot, before, jnp.where(number == long_slot, jnp.int32(MOST), after)))
    lengths = jnp.stack(lengths).astype(jnp.int32)
    ends = jnp.cumsum(lengths).astype(jnp.int32)
    positions = jnp.arange(SEQUENCE_TOKENS, dtype=jnp.int32)
    ids = jnp.sum((positions[:, None] >= ends[None, :DOCS - 1]).astype(jnp.int32), axis=1).astype(jnp.int32)
    starts = ends - lengths
    long_start = jnp.sum(jnp.where(jnp.arange(DOCS, dtype=jnp.int32) == long_slot, starts, 0)).astype(jnp.int32)
    return (ids, long_start)


def draw_token_document(key, part):
    return doc_layout(key)[0]


def draw_codes(key, part):
    return weight_parts(key)[0]


def draw_column_scale_quantized(key, part):
    return weight_parts(key)[1]


def draw_block_second_scale(key, part):
    return weight_parts(key)[2]


def far_pairs(key, fields, weight):
    long_start = doc_layout(key)[1]
    hq_local = QUERY_HEADS // N_FSDP
    key_value_local = KEY_VALUE_HEADS // N_FSDP
    group_columns = COLS // N_FSDP
    head_grouped = QUERY_HEADS // KEY_VALUE_HEADS
    half_size = HEAD_SIZE // 2
    edge_dims = max(HEAD_SIZE // 16, 1)
    aligned = list(range(half_size - edge_dims, half_size)) + list(range(HEAD_SIZE - edge_dims, HEAD_SIZE))
    root_width = math.sqrt(MODEL_WIDTH)
    for plant in range(8):
        query_head = 3 * plant % QUERY_HEADS
        group_id = query_head // hq_local
        key_head = query_head // head_grouped
        query_cols = np.array([group_id * group_columns + (query_head - group_id * hq_local) * HEAD_SIZE + dim for dim in aligned])
        key_cols = np.array([group_id * group_columns + hq_local * HEAD_SIZE + (key_head - group_id * key_value_local) * HEAD_SIZE + dim for dim in aligned])
        columns = jnp.concatenate([weight[:, query_cols], weight[:, key_cols]], axis=1)
        direction = jnp.sum(columns, axis=1)
        direction = direction / jnp.sqrt(jnp.sum(direction * direction))
        offset = jax.random.randint(jax.random.fold_in(key, 500 + plant), (), 0, SEQUENCE_TOKENS // 4, dtype=jnp.int32)
        position = long_start + offset
        vector = root_width * direction
        fields = fields.at[position].set(vector)
        fields = fields.at[position + SEQUENCE_TOKENS // 2].set(vector)
    return fields


def draw_layer_input(key, part):
    fields = jax.random.normal(jax.random.fold_in(key, 201), (SEQUENCE_TOKENS, MODEL_WIDTH), jnp.float32)
    packed, scales, consts = weight_parts(key)
    weight = unpack_weights(packed, scales, consts)
    fields = far_pairs(key, fields, weight)
    return jnp.clip(fields, -6.0, 6.0).astype(jnp.bfloat16)


def shard_levels(stream_key, shape, shards, low, top_value):
    level = 1.0
    for dim, shards_of in shards:
        steps = jax.random.uniform(jax.random.fold_in(jax.random.fold_in(stream_key, 6), dim), (shards_of,), jnp.float32, low / len(shards), top_value / len(shards))
        level = level * jnp.repeat(jnp.exp(steps), shape[dim] // shards_of).reshape((-1,) + (1,) * (len(shape) - 1 - dim))
    return level


def bell_draw(key, dims, width, most, cuts=(), held_as=jnp.bfloat16):
    result = jax.random.normal(key, dims, jnp.float32) * width
    if len(cuts) > 0:
        result = shard_levels(key, dims, cuts, -0.22, 0.18) * result
    return jnp.clip(result, min=-most, max=most).astype(held_as)


def setup_inputs(seed: int = 0) -> dict:
    splits = jax.random.split(jax.random.key(seed), 10)
    layer_input = draw_layer_input(jax.random.fold_in(splits[9], 71), 0)
    gain = jnp.clip(1.0 + 0.1 * jax.random.normal(splits[1], (MODEL_WIDTH,), jnp.float32), 0.5, 1.5)
    codes = draw_codes(jax.random.fold_in(splits[9], 71), 0)
    column_scale_quantized = draw_column_scale_quantized(jax.random.fold_in(splits[9], 71), 0)
    block_second_scale = draw_block_second_scale(jax.random.fold_in(splits[9], 71), 0)
    query_down_map = bell_draw(splits[5], (MODEL_WIDTH, ADAPTER_RANK), MODEL_WIDTH ** -0.5, 0.09375)
    query_up_map = bell_draw(splits[6], (ADAPTER_RANK, QUERY_FEATURES), 0.05, 0.29882812, ((1, 2),))
    token_document = draw_token_document(jax.random.fold_in(splits[9], 71), 0)
    output_cotangent = bell_draw(splits[8], (SEQUENCE_TOKENS, QUERY_FEATURES), 0.01, 0.059814453, ((0, 16), (1, 2)))
    return {"layer_input": layer_input, "gain": gain, "codes": codes, "column_scale_quantized": column_scale_quantized, "block_second_scale": block_second_scale, "query_down_map": query_down_map, "query_up_map": query_up_map, "token_document": token_document, "output_cotangent": output_cotangent}


NF4_LEVELS = [-1.0, -0.6961928009986877, -0.5250730514526367, -0.39491748809814453, -0.28444138169288635, -0.18477343022823334, -0.09105003625154495, 0.0, 0.07958029955625534, 0.16093020141124725, 0.24611230194568634, 0.33791524171829224, 0.44070982933044434, 0.5626170039176941, 0.7229568362236023, 1.0]
ADAPTER_SCALE = 2.0
ROPE_BASE = 500000.0

def dequantize(packed, column_scale_quantized, block_second_scale):
    row_count = packed.shape[0]
    pieces = [jnp.bitwise_and(jnp.right_shift(packed, 4 * nibble), 15) for nibble in range(8)]
    unpacked = jnp.stack(pieces, axis=-1).reshape(row_count, packed.shape[1] * 8)
    levels = jnp.zeros(unpacked.shape, jnp.float32)
    for slot_code, level_value in enumerate(NF4_LEVELS):
        levels = levels + jnp.where(unpacked == slot_code, jnp.float32(level_value), jnp.float32(0.0))
    absmax = (column_scale_quantized.astype(jnp.float32) + 1.0) / 256.0 * block_second_scale[:, None]
    scaled = levels.reshape(row_count // 64, 64, -1) * absmax[:, None, :]
    return scaled.reshape(row_count, -1).astype(jnp.bfloat16)

def rope_angles(positions):
    freqs = jnp.exp(jnp.arange(HEAD_SIZE // 2, dtype=jnp.float32) * (-2.0 * math.log(ROPE_BASE) / HEAD_SIZE))
    angle = positions.astype(jnp.float32)[:, None] * freqs[None, :]
    cosine = jnp.concatenate([jnp.cos(angle), jnp.cos(angle)], axis=-1)
    sine = jnp.concatenate([jnp.sin(angle), jnp.sin(angle)], axis=-1)
    return (cosine, sine)

def apply_rotation(field, rotary_phases):
    cosine, sine = rotary_phases
    half = HEAD_SIZE // 2
    turned = jnp.concatenate([-field[..., half:], field[..., :half]], axis=-1)
    return field * cosine[:, None, :] + turned * sine[:, None, :]

def rotate_back(grads, rotary_phases):
    cosine, sine = rotary_phases
    half = HEAD_SIZE // 2
    scaled = grads * sine[:, None, :]
    turned = jnp.concatenate([-scaled[..., half:], scaled[..., :half]], axis=-1)
    return grads * cosine[:, None, :] - turned

def rms_norm(layer_input, gain):
    wide = layer_input.astype(jnp.float32)
    inverse = lax.rsqrt(lax.optimization_barrier(jnp.mean(wide * wide, axis=-1, keepdims=True)) + 1e-05)
    return (wide * inverse * gain[None, :]).astype(jnp.bfloat16)

def reference(layer_input, gain, codes, column_scale_quantized, block_second_scale, query_down_map, query_up_map, token_document, output_cotangent):
    input_normalized = rms_norm(layer_input, gain)
    weight = dequantize(codes, column_scale_quantized, block_second_scale)
    projection_output = jnp.dot(input_normalized.astype(jnp.float32), weight.astype(jnp.float32), preferred_element_type=jnp.float32)
    group_columns = (QUERY_HEADS + 2 * KEY_VALUE_HEADS) * HEAD_SIZE // N_FSDP
    q_local = QUERY_HEADS // N_FSDP * HEAD_SIZE
    key_value_local = KEY_VALUE_HEADS // N_FSDP * HEAD_SIZE
    query_slices, key_slices, value_slices = ([], [], [])
    for member in range(N_FSDP):
        anchor = member * group_columns
        query_slices.append(projection_output[:, anchor:anchor + q_local])
        key_slices.append(projection_output[:, anchor + q_local:anchor + q_local + key_value_local])
        value_slices.append(projection_output[:, anchor + q_local + key_value_local:anchor + group_columns])
    rank_reduced = jnp.dot(input_normalized.astype(jnp.float32), query_down_map.astype(jnp.float32), preferred_element_type=jnp.float32).astype(jnp.bfloat16)
    query_complete = jnp.concatenate(query_slices, axis=1) + ADAPTER_SCALE * jnp.dot(rank_reduced.astype(jnp.float32), query_up_map.astype(jnp.float32), preferred_element_type=jnp.float32)
    positions = jnp.arange(SEQUENCE_TOKENS, dtype=jnp.int32)
    rotary_phases = rope_angles(positions)
    query_rows = apply_rotation(query_complete.reshape(SEQUENCE_TOKENS, QUERY_HEADS, HEAD_SIZE), rotary_phases).astype(jnp.bfloat16)
    key_rows = apply_rotation(jnp.concatenate(key_slices, axis=1).reshape(SEQUENCE_TOKENS, KEY_VALUE_HEADS, HEAD_SIZE), rotary_phases).astype(jnp.bfloat16)
    value_rows = jnp.concatenate(value_slices, axis=1).reshape(SEQUENCE_TOKENS, KEY_VALUE_HEADS, HEAD_SIZE).astype(jnp.bfloat16)
    head_grouped = QUERY_HEADS // KEY_VALUE_HEADS
    query_grouped = query_rows.reshape(SEQUENCE_TOKENS, KEY_VALUE_HEADS, head_grouped, HEAD_SIZE).astype(jnp.float32)
    grouped_gradient = output_cotangent.reshape(SEQUENCE_TOKENS, KEY_VALUE_HEADS, head_grouped, HEAD_SIZE).astype(jnp.float32)
    keys_wide = key_rows.astype(jnp.float32)
    values_wide = value_rows.astype(jnp.float32)
    soft_scale = 1.0 / math.sqrt(HEAD_SIZE)
    block = math.gcd(SEQUENCE_TOKENS, 256)

    def one_block(block_id):
        start = (block_id * block).astype(jnp.int32)
        query_blk = lax.dynamic_slice_in_dim(query_grouped, start, block, 0)
        grad_blk = lax.dynamic_slice_in_dim(grouped_gradient, start, block, 0)
        ids_blk = lax.dynamic_slice_in_dim(token_document, start, block, 0)
        pos_blk = start + jnp.arange(block, dtype=jnp.int32)
        allowed = (ids_blk[:, None] == token_document[None, :]) & (positions[None, :] <= pos_blk[:, None])
        scores = jnp.einsum('bhgd,shd->hgbs', query_blk, keys_wide) * soft_scale
        masked = jnp.where(allowed, scores, -1e+30)
        top = lax.optimization_barrier(jnp.max(masked, axis=-1, keepdims=True))
        expo = jnp.where(allowed, jnp.exp(masked - top), 0.0)
        probs = expo / lax.optimization_barrier(jnp.sum(expo, axis=-1, keepdims=True))
        rounded = probs.astype(jnp.bfloat16).astype(jnp.float32)
        output = jnp.einsum('hgbs,shd->bhgd', rounded, values_wide)
        grad_dots = jnp.einsum('bhgd,shd->hgbs', grad_blk, values_wide)
        mean_dot = lax.optimization_barrier(jnp.sum(probs * grad_dots, axis=-1, keepdims=True))
        grad_scores = (probs * (grad_dots - mean_dot)).astype(jnp.bfloat16).astype(jnp.float32)
        grad_query = jnp.einsum('hgbs,shd->bhgd', grad_scores, keys_wide) * soft_scale
        return (output, grad_query)
    outputs, grad_queries = lax.map(one_block, jnp.arange(SEQUENCE_TOKENS // block, dtype=jnp.int32))
    attn = outputs.reshape(SEQUENCE_TOKENS, QUERY_HEADS * HEAD_SIZE).astype(jnp.bfloat16)
    linear_gradient = rotate_back(grad_queries.reshape(SEQUENCE_TOKENS, QUERY_HEADS, HEAD_SIZE), rotary_phases).reshape(SEQUENCE_TOKENS, QUERY_HEADS * HEAD_SIZE).astype(jnp.bfloat16)
    up_map_gradient = ADAPTER_SCALE * jnp.dot(rank_reduced.T.astype(jnp.float32), linear_gradient.astype(jnp.float32), preferred_element_type=jnp.float32)
    middle_gradient = (ADAPTER_SCALE * jnp.dot(linear_gradient.astype(jnp.float32), query_up_map.T.astype(jnp.float32), preferred_element_type=jnp.float32)).astype(jnp.bfloat16)
    grad_a = jnp.dot(input_normalized.T.astype(jnp.float32), middle_gradient.astype(jnp.float32), preferred_element_type=jnp.float32)
    return (attn, grad_a, up_map_gradient)
```

```python
import math
import functools

import jax
import jax.numpy as jnp
from jax import lax
from jax.experimental import pallas as pl
from jax.experimental.pallas import tpu as pltpu
from jax.sharding import PartitionSpec as P

QUERY_HEADS = 16
KEY_VALUE_HEADS = 4
HEAD_SIZE = 128
ADAPTER_SCALE = 2.0
ROPE_BASE = 500000.0
ID_ROWS = 16
MESH = pl.DeviceIdType.MESH
F32 = jnp.float32
BF16 = jnp.bfloat16

NF4_LEVELS = [
    -1.0,
    -0.6961928009986877,
    -0.5250730514526367,
    -0.39491748809814453,
    -0.28444138169288635,
    -0.18477343022823334,
    -0.09105003625154495,
    0.0,
    0.07958029955625534,
    0.16093020141124725,
    0.24611230194568634,
    0.33791524171829224,
    0.44070982933044434,
    0.5626170039176941,
    0.7229568362236023,
    1.0,
]


def take_lanes(values, index):
    return jnp.take_along_axis(values, index, axis=1, mode="promise_in_bounds")


def nt(a, b):
    return lax.dot_general(a, b, (((1,), (1,)), ((), ())), preferred_element_type=F32)


def tn(a, b):
    return lax.dot_general(a, b, (((0,), (0,)), ((), ())), preferred_element_type=F32)


def proj_kernel(
    x_ref, gain_ref, codes_ref, cs_ref, bss_ref, qdown_ref, qup_ref, ids_ref, cos_ref, sin_ref,
    q_ref, kv_ref, xn_ref, lr_ref,
    scl, vscl, acc, acct, own_kv, send_kv, recv_kv, send_q, recv_q, send_sem, recv_sem,
):
    member = lax.axis_index("fsdp")
    partner = 1 - member
    rows = x_ref.shape[0]
    width = x_ref.shape[1]
    depth = codes_ref.shape[0]
    blocks = cs_ref.shape[0]
    block_rows = depth // blocks
    half_lanes = 64

    barrier = pltpu.get_barrier_semaphore()
    pl.semaphore_signal(barrier, inc=1, device_id={"fsdp": partner}, device_id_type=MESH)
    pl.semaphore_wait(barrier, 1)

    lane = lax.broadcasted_iota(jnp.int32, (blocks, 128), 1)
    second = bss_ref[pl.ds(pl.multiple_of(member * blocks, 8), blocks), :]
    for tile in range(3):
        source = [
            (cs_ref[:, tile * 1024 + m * 128 : tile * 1024 + (m + 1) * 128].astype(F32) + 1.0)
            / 256.0
            * second
            for m in range(8)
        ]
        for n in range(8):
            index = 8 * (lane % 16) + n
            picked = take_lanes(source[0], index)
            for m in range(1, 8):
                picked = jnp.where(lane // 16 == m, take_lanes(source[m], index), picked)
            scl[tile * 8 + n] = picked

    for r in range(0, rows, 16):
        wide = x_ref[r : r + 16, :].astype(F32)
        inverse = lax.rsqrt(jnp.mean(wide * wide, axis=-1, keepdims=True) + 1e-05)
        xn_ref[r : r + 16, :] = (wide * inverse * gain_ref[...]).astype(BF16)
    lr_t = nt(qdown_ref[...], xn_ref[...]).astype(BF16)
    lr_ref[...] = lr_t

    level_lane = lax.broadcasted_iota(jnp.int32, (block_rows, 128), 1)
    table = jnp.zeros((block_rows, 128), F32)
    for code, level in enumerate(NF4_LEVELS):
        table = jnp.where(level_lane % 16 == code, F32(level), table)
    low_lanes = level_lane < half_lanes

    pr = lax.broadcasted_iota(jnp.int32, (128, 128), 0)
    pd = lax.broadcasted_iota(jnp.int32, (128, 128), 1)
    perm = (pd == 8 * (pr % 16) + pr // 16).astype(F32).astype(BF16)

    chunk = 512
    per_chunk = chunk // block_rows

    def phase(low_tile, high_tile):
        low_at = pl.multiple_of(low_tile * 128, 128)
        high_at = pl.multiple_of(high_tile * 128, 128)
        for n in range(8):
            vscl[n] = jnp.where(
                lane < half_lanes, scl[low_tile * 8 + n], scl[high_tile * 8 + n]
            )
        acc[...] = jnp.zeros_like(acc)

        def step(k, carry):
            lhs = xn_ref[:, pl.ds(pl.multiple_of(member * depth + k * chunk, 128), chunk)]
            words = []
            for b in range(per_chunk):
                at = pl.multiple_of(k * chunk + b * block_rows, block_rows)
                words.append(
                    jnp.where(
                        low_lanes,
                        codes_ref[pl.ds(at, block_rows), pl.ds(low_at, 128)],
                        codes_ref[pl.ds(at, block_rows), pl.ds(high_at, 128)],
                    )
                )
            for pair in range(4):
                planes = []
                for n in (2 * pair, 2 * pair + 1):
                    pieces = []
                    for b in range(per_chunk):
                        code = jnp.bitwise_and(jnp.right_shift(words[b], 4 * n), 15)
                        scale = vscl[n, pl.ds(k * per_chunk + b, 1), :]
                        pieces.append((take_lanes(table, code) * scale).astype(BF16))
                    planes.append(jnp.concatenate(pieces, axis=0))
                weight = jnp.concatenate(planes, axis=1)
                acc[:, pair * 256 : (pair + 1) * 256] += jnp.dot(
                    lhs, weight, preferred_element_type=F32
                )
            return carry

        lax.fori_loop(0, depth // chunk, step, 0)

    def turn(out):
        for n in range(8):
            out[n] = acc[:, n * 128 : (n + 1) * 128].T

    def exchange(src, dst, number):
        copy = pltpu.make_async_remote_copy(
            src_ref=src,
            dst_ref=dst,
            send_sem=send_sem.at[number],
            recv_sem=recv_sem.at[number],
            device_id={"fsdp": partner},
            device_id_type=MESH,
        )
        copy.start()
        return copy

    phase(1, 2)
    turn(acct)
    own_at = pl.multiple_of(member * 64, 64)
    other_at = pl.multiple_of(partner * 64, 64)
    send_kv[...] = acct[:, pl.ds(other_at, 64), :].astype(BF16)
    copy_kv = exchange(send_kv, recv_kv, 0)
    own_kv[...] = acct[:, pl.ds(own_at, 64), :]

    phase(2 * partner, partner)
    turn(acct)
    send_q[...] = acct[...].astype(BF16)
    copy_q = exchange(send_q, recv_q, 1)

    cosine = cos_ref[...].reshape(8, 8, rows)
    sine = sin_ref[...].reshape(8, 8, rows)

    def rotate(field):
        a, b = field[:, :8, :], field[:, 8:, :]
        return jnp.concatenate([a * cosine - b * sine, b * cosine + a * sine], axis=1)

    def natural(field):
        return tn(field.reshape(128, rows).astype(BF16), perm).astype(BF16)

    copy_kv.wait()
    for head in range(2):
        k_at, v_at = 16 * head, 32 + 16 * head
        key = own_kv[:, k_at : k_at + 16, :] + recv_kv[:, k_at : k_at + 16, :].astype(F32)
        kv_ref[:rows, head * 256 : head * 256 + 128] = natural(rotate(key))
        value = own_kv[:, v_at : v_at + 16, :] + recv_kv[:, v_at : v_at + 16, :].astype(F32)
        kv_ref[:rows, head * 256 + 128 : head * 256 + 256] = natural(value)
    ids = jnp.broadcast_to(ids_ref[...].astype(F32), (ID_ROWS, rows)).astype(BF16)
    kv_ref[rows:, :] = jnp.concatenate([ids] * 4, axis=1)

    phase(2 * member, member)
    turn(acct)
    copy_q.wait()
    for head in range(8):
        at = pl.multiple_of(16 * lax.rem(head + 4 * member, 8), 16)
        up_t = nt(perm, qup_ref[:, head * 128 : (head + 1) * 128]).astype(BF16)
        adapter = jnp.dot(up_t, lr_t, preferred_element_type=F32).reshape(8, 16, rows)
        query = acct[:, pl.ds(at, 16), :] + recv_q[:, pl.ds(at, 16), :].astype(F32)
        query = query + ADAPTER_SCALE * adapter
        q_ref[:, head * 128 : (head + 1) * 128] = natural(rotate(query))


def attn_kernel(
    first_ref, q_ref, do_ref, kv_ref, ids_ref, xn_ref, lr_ref, qup_ref, cos_ref, sin_ref,
    out_ref, up_ref, ga_ref,
    qs, dos, row_max, row_sum, row_dot, out_acc, grad_acc, lin,
):
    me = lax.axis_index("ctx")
    rows = q_ref.shape[0]
    soft_scale = 1.0 / math.sqrt(HEAD_SIZE)
    group = QUERY_HEADS // KEY_VALUE_HEADS
    many = group * rows
    my_ids = ids_ref[...]

    for head in range(8):
        at = head * rows
        qs[at : at + rows, :] = q_ref[:, head * 128 : (head + 1) * 128]
        dos[at : at + rows, :] = do_ref[:, head * 128 : (head + 1) * 128]

    def part(head, kv_part, allowed, first):
        span = pl.ds(head * many, many)
        key = kv_part[:, head * 256 : head * 256 + 128]
        value = kv_part[:, head * 256 + 128 : head * 256 + 256]
        both = kv_part[:, head * 256 : head * 256 + 256]
        scores = nt(qs[span, :], key) * soft_scale
        scores = jnp.where(jnp.concatenate([allowed] * group, axis=0), scores, -1e30)
        top = jnp.max(scores, axis=-1, keepdims=True)
        if not first:
            top = jnp.maximum(top, row_max[span, :])
        expo = jnp.exp(scores - top)
        weighted = expo * nt(dos[span, :], value)
        total = jnp.sum(expo, axis=-1, keepdims=True)
        dot_total = jnp.sum(weighted, axis=-1, keepdims=True)
        new_out = jnp.dot(expo.astype(BF16), both, preferred_element_type=F32)
        new_grad = jnp.dot(weighted.astype(BF16), key, preferred_element_type=F32)
        if first:
            row_sum[span, :] = total
            row_dot[span, :] = dot_total
            out_acc[span, :] = new_out
            grad_acc[span, :] = new_grad
        else:
            decay = jnp.exp(row_max[span, :] - top)
            row_sum[span, :] = decay * row_sum[span, :] + total
            row_dot[span, :] = decay * row_dot[span, :] + dot_total
            out_acc[span, :] = decay * out_acc[span, :] + new_out
            grad_acc[span, :] = decay * grad_acc[span, :] + new_grad
        row_max[span, :] = top

    diag = kv_ref[me]
    key_ids = diag[rows : rows + 1, :128].astype(F32)
    qi = lax.broadcasted_iota(jnp.int32, (rows, rows), 0)
    ki = lax.broadcasted_iota(jnp.int32, (rows, rows), 1)
    allowed = (my_ids == key_ids) & (ki <= qi)
    for head in range(2):
        part(head, diag[:rows], allowed, True)

    lane = lax.broadcasted_iota(jnp.int32, (1, 2 * rows), 1)

    def step(t, carry):
        upper = me - 2 * t
        start = jnp.maximum(upper - 2, 0)
        pair = [kv_ref[start], kv_ref[start + 1]]
        both = jnp.concatenate([p[:rows] for p in pair], axis=0)
        key_ids = jnp.concatenate([p[rows : rows + 1, :128] for p in pair], axis=1).astype(F32)
        key_ids = jnp.where(lane < (upper - start) * rows, key_ids, -1.0)
        allowed = my_ids == key_ids
        for head in range(2):
            part(head, both, allowed, False)
        return carry

    lax.fori_loop(0, (me - first_ref[0] + 1) // 2, step, 0)

    cosine, sine = cos_ref[...], sin_ref[...]
    for head in range(8):
        at = head * rows
        span = slice(at, at + rows)
        inverse = 1.0 / row_sum[span, :]
        out_ref[:, head * 128 : (head + 1) * 128] = (out_acc[span, 128:] * inverse).astype(BF16)
        mean_dot = row_dot[span, :] * inverse
        grad = soft_scale * inverse * (grad_acc[span, :] - mean_dot * out_acc[span, :128])
        turned = pltpu.roll(grad * sine, 64, 1)
        lin[:, head * 128 : (head + 1) * 128] = (grad * cosine + turned).astype(BF16)
    up_ref[...] = ADAPTER_SCALE * jnp.dot(lr_ref[...], lin[...], preferred_element_type=F32)
    middle = (ADAPTER_SCALE * nt(qup_ref[...], lin[...])).astype(BF16)
    ga_ref[...] = jnp.dot(middle, xn_ref[...], preferred_element_type=F32)


def rope_tables(place, rows):
    positions = (place * rows + jnp.arange(rows, dtype=jnp.int32)).astype(F32)
    half = HEAD_SIZE // 2
    freqs = jnp.exp(jnp.arange(half, dtype=F32) * (-2.0 * math.log(ROPE_BASE) / HEAD_SIZE))
    angle = positions[:, None] * freqs[None, :]
    cosine, sine = jnp.cos(angle), jnp.sin(angle)
    def planes(table):
        return jnp.transpose(table.T.reshape(8, 8, rows), (1, 0, 2)).reshape(half, rows)

    wide_cos = jnp.concatenate([cosine, cosine], axis=-1)
    wide_sin = jnp.concatenate([-sine, sine], axis=-1)
    return planes(cosine), planes(sine), wide_cos, wide_sin


def on_device(
    layer_input, gain, codes, column_scale_quantized, block_second_scale,
    query_down_map, query_up_map, token_document, output_cotangent,
):
    rows, width = layer_input.shape
    place = lax.axis_index("ctx")
    cos_t, sin_t, cos_w, sin_w = rope_tables(place, rows)
    vm = pl.BlockSpec(memory_space=pltpu.VMEM)
    sm = pl.BlockSpec(memory_space=pltpu.SMEM)
    blocks = column_scale_quantized.shape[0]
    rank = query_up_map.shape[0]
    kv_width = 4 * HEAD_SIZE
    q, kv, xn, lr = pl.pallas_call(
        proj_kernel,
        out_shape=(
            jax.ShapeDtypeStruct((rows, query_up_map.shape[1]), BF16),
            jax.ShapeDtypeStruct((rows + ID_ROWS, kv_width), BF16),
            jax.ShapeDtypeStruct((rows, width), BF16),
            jax.ShapeDtypeStruct((rank, rows), BF16),
        ),
        in_specs=[vm] * 10,
        out_specs=(vm,) * 4,
        scratch_shapes=[
            pltpu.VMEM((24, blocks, 128), F32),
            pltpu.VMEM((8, blocks, 128), F32),
            pltpu.VMEM((rows, 1024), F32),
            pltpu.VMEM((8, 128, rows), F32),
            pltpu.VMEM((8, 64, rows), F32),
            pltpu.VMEM((8, 64, rows), BF16),
            pltpu.VMEM((8, 64, rows), BF16),
            pltpu.VMEM((8, 128, rows), BF16),
            pltpu.VMEM((8, 128, rows), BF16),
            pltpu.SemaphoreType.DMA((2,)),
            pltpu.SemaphoreType.DMA((2,)),
        ],
        compiler_params=pltpu.CompilerParams(
            collective_id=0, has_side_effects=True, vmem_limit_bytes=56 * 1024 * 1024
        ),
        name="project",
    )(
        layer_input, gain[None, :], codes, column_scale_quantized, block_second_scale[:, None],
        query_down_map.T, query_up_map, token_document[None, :], cos_t, sin_t,
    )
    all_kv = lax.all_gather(kv, "ctx", axis=0, tiled=False)
    all_ids = all_kv[:, rows, :rows].astype(F32)
    needed = (all_ids[:, -1] >= token_document[0].astype(F32)) & (
        jnp.arange(all_ids.shape[0]) <= place
    )
    first = jnp.argmax(needed).astype(jnp.int32)[None]
    heads_rows = 8 * rows
    attn, up, ga = pl.pallas_call(
        attn_kernel,
        out_shape=(
            jax.ShapeDtypeStruct(output_cotangent.shape, BF16),
            jax.ShapeDtypeStruct(query_up_map.shape, F32),
            jax.ShapeDtypeStruct((rank, width), F32),
        ),
        in_specs=[sm] + [vm] * 9,
        out_specs=(vm,) * 3,
        scratch_shapes=[
            pltpu.VMEM((heads_rows, 128), BF16),
            pltpu.VMEM((heads_rows, 128), BF16),
            pltpu.VMEM((heads_rows, 1), F32),
            pltpu.VMEM((heads_rows, 1), F32),
            pltpu.VMEM((heads_rows, 1), F32),
            pltpu.VMEM((heads_rows, 256), F32),
            pltpu.VMEM((heads_rows, 128), F32),
            pltpu.VMEM((rows, 1024), BF16),
        ],
        compiler_params=pltpu.CompilerParams(vmem_limit_bytes=56 * 1024 * 1024),
        name="attend",
    )(
        first, q, output_cotangent, all_kv, token_document.astype(F32)[:, None], xn, lr,
        query_up_map, cos_w, sin_w,
    )
    up = lax.psum(up, "ctx")
    ga = lax.psum(ga, ("ctx", "fsdp"))
    return attn, ga.T, up


def solution(mesh):
    return jax.shard_map(
        on_device,
        mesh=mesh,
        in_specs=(
            P("ctx", None),
            P(),
            P("fsdp", None),
            P("fsdp", None),
            P(),
            P(),
            P(None, "fsdp"),
            P("ctx"),
            P("ctx", "fsdp"),
        ),
        out_specs=(P("ctx", "fsdp"), P(), P(None, "fsdp")),
        check_vma=False,
    )
```
